32 devices in a mesh: dp: 8 (over z, x), mp: 4 (over y, core).
Axes of the slice: x: 2, y: 2, z: 4, core: 2. Of those that a mesh axis runs over, the one named last changes fastest.
Arguments:
- token_ids: int32 [8, 1024], P('dp'), may hold values from 0 to 50303
- target_ids: int32 [8, 1024], P('dp'), may hold values from 0 to 50303
- segment_ids: int32 [8, 1024], P('dp'), may hold values from 0 to 3, never falling along the last dimension, each value on 1 to 512 neighbouring positions
- domain_ids: int32 [8, 1024], P('dp'), may hold values from 0 to 7, as said below
- domain_weights: int32 [8], replicated, may hold values from 1 to 8
- table: float32 [50304, 1024], P(('dp', 'mp')), may hold values from -0.375 to 0.375
- attn_weights: float32 [4, 1024, 1024], P(None, 'dp', 'mp'), may hold values from -0.1875 to 0.1875
- out_weights: float32 [1024, 1024], P('mp', 'dp'), may hold values from -0.1875 to 0.1875
- ffn_weights: float32 [2, 1024, 2816], P(None, 'dp', 'mp'), may hold values from -0.1875 to 0.1875
- down_weights: float32 [2816, 1024], P('mp', 'dp'), may hold values from -0.02734375 to 0.02734375
- gains: float32 [4, 1024], P(None, 'dp'), may hold values from 0.5 to 1.5
- table_moment: float32 [50304, 1024], P(('dp', 'mp')), may hold values from -0.00018310547 to 0.00018310547
- attn_moment: float32 [4, 1024, 1024], P(None, 'dp', 'mp'), may hold values from -0.00018310547 to 0.00018310547
- out_moment: float32 [1024, 1024], P('mp', 'dp'), may hold values from -0.00018310547 to 0.00018310547
- ffn_moment: float32 [2, 1024, 2816], P(None, 'dp', 'mp'), may hold values from -0.00018310547 to 0.00018310547
- down_moment: float32 [2816, 1024], P('mp', 'dp'), may hold values from -0.00018310547 to 0.00018310547
- gain_moment: float32 [4, 1024], P(None, 'dp'), may hold values from -0.0009765625 to 0.0009765625
- table_average: float32 [50304, 1024], P(('dp', 'mp')), may hold values from -0.375 to 0.375
- attn_average: float32 [4, 1024, 1024], P(None, 'dp', 'mp'), may hold values from -0.1875 to 0.1875
- out_average: float32 [1024, 1024], P('mp', 'dp'), may hold values from -0.1875 to 0.1875
- ffn_average: float32 [2, 1024, 2816], P(None, 'dp', 'mp'), may hold values from -0.1875 to 0.1875
- down_average: float32 [2816, 1024], P('mp', 'dp'), may hold values from -0.02734375 to 0.02734375
- gain_average: float32 [4, 1024], P(None, 'dp'), may hold values from 0.5 to 1.5
Outputs:
- total_loss: float32 [], replicated
- domain_loss: float32 [8], replicated
- grad_norm: float32 [], replicated
- new_table_moment: float32 [50304, 1024], P(('dp', 'mp'))
- new_table: float32 [50304, 1024], P(('dp', 'mp'))
- new_table_average: float32 [50304, 1024], P(('dp', 'mp'))
- new_attn_moment: float32 [4, 1024, 1024], P(None, 'dp', 'mp')
- new_attn: float32 [4, 1024, 1024], P(None, 'dp', 'mp')
- new_attn_average: float32 [4, 1024, 1024], P(None, 'dp', 'mp')
- new_out_moment: float32 [1024, 1024], P('mp', 'dp')
- new_out: float32 [1024, 1024], P('mp', 'dp')
- new_out_average: float32 [1024, 1024], P('mp', 'dp')
- new_ffn_moment: float32 [2, 1024, 2816], P(None, 'dp', 'mp')
- new_ffn: float32 [2, 1024, 2816], P(None, 'dp', 'mp')
- new_ffn_average: float32 [2, 1024, 2816], P(None, 'dp', 'mp')
- new_down_moment: float32 [2816, 1024], P('mp', 'dp')
- new_down: float32 [2816, 1024], P('mp', 'dp')
- new_down_average: float32 [2816, 1024], P('mp', 'dp')
- new_gain_moment: float32 [4, 1024], P(None, 'dp')
- new_gains: float32 [4, 1024], P(None, 'dp')
- new_gain_average: float32 [4, 1024], P(None, 'dp')
The draws below stay inside these ranges and needn't reach their ends.
Inputs may be any that keep to these rules, and one draw needn't show every extreme that they name: `segment_ids`: segment ids never fall along a sequence; each sequence holds 4 documents. `domain_ids`: A domain may hold no token at all.
All inputs are finite; a program needn't handle non-finite values.
Results may differ from the reference program's by a relative error of at most 0.0083.
Values may be sent and summed in bfloat16 or wider, within the bound.
A program may use at most 320 MiB of HBM per device.

```python
import math
import jax
import jax.numpy as jnp
import numpy as np
from jax import lax

D = 1024
H = 16
HD = 64
FF = 2816
VOCAB = 50304
TOK_DEV = 1024
DOCS = 4
DOMAINS = 8
SEQS = 8


def draw_domain_ids(key, part):
    absent_domain = jax.random.randint(jax.random.fold_in(key, 11), (), 1, DOMAINS - 1)
    drawn = jax.random.randint(jax.random.fold_in(key, 12), (SEQS, TOK_DEV), 0, DOMAINS - 1)
    domain_rows = drawn + (drawn >= absent_domain).astype(jnp.int32)
    domain_rows = domain_rows.at[0, 0].set(0)
    domain_rows = domain_rows.at[0, 1].set(DOMAINS - 1)
    return domain_rows.astype(jnp.int32)


def plant(array, stream_key, smallest, top_value):
    spot = [jax.random.randint(jax.random.fold_in(stream_key, axis), (), 0, length) for axis, length in enumerate(array.shape)]
    widest = array.shape.index(max(array.shape))
    neighbour = spot[:widest] + [(spot[widest] + 1) % array.shape[widest]] + spot[widest + 1:]
    return array.at[tuple(spot)].set(smallest).at[tuple(neighbour)].set(top_value)


def steps_of(rng, dims, cuts, least, high):
    factor_of, own = 1.0, jax.random.fold_in(rng, 6)
    for position, blocks in cuts:
        heights = jnp.exp(jax.random.uniform(jax.random.fold_in(own, position), (blocks,), jnp.float32, least / len(cuts), high / len(cuts)))
        factor_of = factor_of * jnp.repeat(heights, dims[position] // blocks).reshape([-1 if axis == position else 1 for axis in range(len(dims))])
    return factor_of


def rank_bounds(count, skew):
    loads = [(1 << 20) // math.isqrt(rank ** skew) + 1 for rank in range(1, count + 1)]
    width = 1 + sum(loads) // (1 << 30)
    return np.cumsum(np.array([max(1, weight // width) for weight in loads]))


def skewed_ids(own_key, shape, count, lean):
    table = rank_bounds(count, lean)
    lot = jax.random.randint(jax.random.fold_in(own_key, 1), shape, 0, int(table[count - 1]))
    grade = jnp.searchsorted(jnp.asarray(table, jnp.int32), lot, side="right")
    return jax.random.permutation(jax.random.fold_in(own_key, 2), count)[grade].astype(jnp.int32)


def split_up(number_of, total, limit, lean):
    portions = [(1 << 20) // math.isqrt(standing ** lean) + 1 for standing in range(2, number_of + 1)]
    spare, holding = total - limit - (number_of - 1), [1] * (number_of - 1)
    while spare > 0:
        free = [i for i in range(number_of - 1) if holding[i] < limit]
        mass, remaining = sum([portions[i] for i in free]), spare
        for i in free:
            more = min(limit - holding[i], max(1, remaining * portions[i] // mass), spare)
            holding[i] = holding[i] + more
            spare = spare - more
    return np.array([limit] + holding)


def ragged_sizes(own_key, amount, total, reach, slope):
    if amount == 2:
        one = jax.random.randint(own_key, (), max(1, total - reach), min(reach, total - 1) + 1)
        return jnp.stack([one, total - one])
    sizes = jnp.asarray(split_up(amount, total, reach, slope), jnp.int32)
    twos = (amount - 1) // 2
    giver, receiver = sizes[1:1 + 2 * twos:2], sizes[2:2 + 2 * twos:2]
    margin = jnp.minimum(giver - 1, reach - receiver)
    passed = jax.random.randint(jax.random.fold_in(own_key, 1), (twos,), 0, 1 << 20) % (margin + 1)
    sizes = sizes.at[1:1 + 2 * twos:2].set(giver - passed).at[2:2 + 2 * twos:2].set(receiver + passed)
    return sizes[jax.random.permutation(jax.random.fold_in(own_key, 2), amount)]


def gaussian(own_key, dims, deviation, reach, split=(), held_as=jnp.bfloat16):
    array = deviation * jax.random.normal(own_key, dims, jnp.float32)
    if split:
        array = array * steps_of(own_key, dims, split, -0.22, 0.18)
    return jnp.clip(array, -reach, reach).astype(held_as)


def setup_inputs(seed: int = 0) -> dict:
    arg_keys = jax.random.split(jax.random.key(seed), 24)
    token_ids = plant(skewed_ids(arg_keys[0], (SEQS, TOK_DEV), VOCAB, 2), jax.random.fold_in(arg_keys[0], 3), 0, VOCAB - 1).astype(jnp.int32)
    target_ids = plant(skewed_ids(arg_keys[1], (SEQS, TOK_DEV), VOCAB, 2), jax.random.fold_in(arg_keys[1], 3), 0, VOCAB - 1).astype(jnp.int32)
    segment_ids = jax.vmap(lambda own: jnp.searchsorted(jnp.cumsum(ragged_sizes(own, DOCS, TOK_DEV, TOK_DEV // 2, 1)), jnp.arange(TOK_DEV), side="right"))(jax.random.split(arg_keys[2], SEQS)).reshape((SEQS, TOK_DEV)).astype(jnp.int32)
    domain_ids = draw_domain_ids(jax.random.fold_in(arg_keys[23], 71), 0)
    domain_weights = plant(jax.random.randint(arg_keys[4], (DOMAINS,), 1, 9), jax.random.fold_in(arg_keys[4], 1), 1, 8).astype(jnp.int32)
    table = gaussian(arg_keys[5], (VOCAB, D), (D // 4) ** -0.5, 0.375, ((0, 32),), jnp.float32)
    attn_weights = gaussian(arg_keys[6], (4, D, D), D ** -0.5, 0.1875, ((1, 8), (2, 4)), jnp.float32)
    out_weights = gaussian(arg_keys[7], (D, D), D ** -0.5, 0.1875, ((0, 4), (1, 8)), jnp.float32)
    ffn_weights = gaussian(arg_keys[8], (2, D, FF), D ** -0.5, 0.1875, ((1, 8), (2, 4)), jnp.float32)
    down_weights = gaussian(arg_keys[9], (FF, D), (16 * FF) ** -0.5, 0.02734375, ((0, 4), (1, 8)), jnp.float32)
    gains = jnp.clip(1.0 + 0.1 * jax.random.normal(arg_keys[10], (4, D), jnp.float32), 0.5, 1.5)
    table_moment = gaussian(arg_keys[11], (VOCAB, D), (0.1 / (VOCAB * D + 5 * D * D + 3 * D * FF) ** 0.5), 0.00018310547, ((0, 32),), jnp.float32)
    attn_moment = gaussian(arg_keys[12], (4, D, D), (0.1 / (VOCAB * D + 5 * D * D + 3 * D * FF) ** 0.5), 0.00018310547, ((1, 8), (2, 4)), jnp.float32)
    out_moment = gaussian(arg_keys[13], (D, D), (0.1 / (VOCAB * D + 5 * D * D + 3 * D * FF) ** 0.5), 0.00018310547, ((0, 4), (1, 8)), jnp.float32)
    ffn_moment = gaussian(arg_keys[14], (2, D, FF), (0.1 / (VOCAB * D + 5 * D * D + 3 * D * FF) ** 0.5), 0.00018310547, ((1, 8), (2, 4)), jnp.float32)
    down_moment = gaussian(arg_keys[15], (FF, D), (0.1 / (VOCAB * D + 5 * D * D + 3 * D * FF) ** 0.5), 0.00018310547, ((0, 4), (1, 8)), jnp.float32)
    gain_moment = gaussian(arg_keys[16], (4, D), (0.5 / (VOCAB * D + 5 * D * D + 3 * D * FF) ** 0.5), 0.0009765625, ((1, 8),), jnp.float32)
    table_average = gaussian(arg_keys[17], (VOCAB, D), (D // 4) ** -0.5, 0.375, ((0, 32),), jnp.float32)
    attn_average = gaussian(arg_keys[18], (4, D, D), D ** -0.5, 0.1875, ((1, 8), (2, 4)), jnp.float32)
    out_average = gaussian(arg_keys[19], (D, D), D ** -0.5, 0.1875, ((0, 4), (1, 8)), jnp.float32)
    ffn_average = gaussian(arg_keys[20], (2, D, FF), D ** -0.5, 0.1875, ((1, 8), (2, 4)), jnp.float32)
    down_average = gaussian(arg_keys[21], (FF, D), (16 * FF) ** -0.5, 0.02734375, ((0, 4), (1, 8)), jnp.float32)
    gain_average = jnp.clip(1.0 + 0.1 * jax.random.normal(arg_keys[22], (4, D), jnp.float32), 0.5, 1.5)
    return dict(token_ids=token_ids, target_ids=target_ids, segment_ids=segment_ids, domain_ids=domain_ids, domain_weights=domain_weights, table=table, attn_weights=attn_weights, out_weights=out_weights, ffn_weights=ffn_weights, down_weights=down_weights, gains=gains, table_moment=table_moment, attn_moment=attn_moment, out_moment=out_moment, ffn_moment=ffn_moment, down_moment=down_moment, gain_moment=gain_moment, table_average=table_average, attn_average=attn_average, out_average=out_average, ffn_average=ffn_average, down_average=down_average, gain_average=gain_average)


EPSILON = 1e-06
CLIP_NORM = 0.01
LEARN_RATE = 1000.0
MOMENTUM = 0.9
AVERAGE_KEEP = 0.75
HIGHEST = lax.Precision.HIGHEST

@jax.custom_vjp
def low(v):
    return lax.optimization_barrier(v.astype(jnp.bfloat16)).astype(jnp.float32)

@jax.custom_vjp
def low_back(v):
    return v

def low_keep(v):
    return (low(v), None)

def low_pass(kept, grad):
    return (grad,)

def back_keep(v):
    return (v, None)

def back_low(kept, grad):
    return (low(grad),)
low.defvjp(low_keep, low_pass)
low_back.defvjp(back_keep, back_low)

def normed(values, gain):
    return values * lax.rsqrt(lax.optimization_barrier(jnp.mean(values * values, axis=-1, keepdims=True)) + EPSILON) * gain

def rotary_tables(length, half):
    places = jnp.arange(length, dtype=jnp.float32)[:, None]
    speeds = 10000.0 ** (-jnp.arange(half, dtype=jnp.float32) / half)
    angles = places * speeds
    return (jnp.cos(angles)[:, None, :], jnp.sin(angles)[:, None, :])

def rotate(values, cosine, sine):
    half = values.shape[-1] // 2
    first = values[..., :half]
    second = values[..., half:]
    return jnp.concatenate([first * cosine - second * sine, second * cosine + first * sine], axis=-1)

def sequence_terms(weights, token_row, target_row, segment_row, domain_row):
    table, attn_w, out_w, ffn_w, down_w, gain_rows = weights
    length = token_row.shape[0]
    embedded = jnp.take(table, token_row, axis=0)
    first_in = low(normed(embedded, gain_rows[0]))
    value_first = low(jnp.dot(first_in, attn_w[3], precision=HIGHEST))
    attn_in = low(normed(embedded, gain_rows[1]))
    cosine, sine = rotary_tables(length, HD // 2)
    queries = low(rotate(low_back(jnp.dot(attn_in, attn_w[0], precision=HIGHEST)).reshape(length, H, HD), cosine, sine))
    keys = low(rotate(low_back(jnp.dot(attn_in, attn_w[1], precision=HIGHEST)).reshape(length, H, HD), cosine, sine))
    values = low_back(low(0.5 * jnp.dot(attn_in, attn_w[2], precision=HIGHEST) + 0.5 * value_first)).reshape(length, H, HD)
    places = jnp.arange(length)
    allowed = (places[:, None] >= places[None, :]) & (segment_row[:, None] == segment_row[None, :])
    scores = low_back(jnp.einsum('qhd,khd->hqk', queries, keys, precision=HIGHEST) * HD ** (-0.5))
    soft_probs = jax.nn.softmax(jnp.where(allowed[None], scores, -1e+30), axis=-1)
    mixed = jnp.einsum('hqk,khd->qhd', low(soft_probs), values, precision=HIGHEST).reshape(length, D)
    mixed = low_back(low(mixed))
    residual_one = embedded + low_back(jnp.dot(mixed, out_w, precision=HIGHEST))
    ffn_in = low(normed(residual_one, gain_rows[2]))
    gate_part = low_back(jnp.dot(ffn_in, ffn_w[0], precision=HIGHEST))
    up_part = low_back(jnp.dot(ffn_in, ffn_w[1], precision=HIGHEST))
    activated = low(jax.nn.silu(gate_part) * up_part)
    residual_two = residual_one + low_back(jnp.dot(activated, down_w, precision=HIGHEST))
    final_in = low(normed(residual_two, gain_rows[3]))
    logits = low_back(jnp.dot(final_in, table.T, precision=HIGHEST))
    row_lse = jax.nn.logsumexp(logits, axis=-1)
    target_logit = jnp.take_along_axis(logits, target_row[:, None], axis=1)[:, 0]
    token_loss = row_lse - target_logit
    matches = domain_row[:, None] == jnp.arange(DOMAINS)[None, :]
    return lax.optimization_barrier(jnp.sum(jnp.where(matches, token_loss[:, None], 0.0), axis=0))

def reference(token_ids, target_ids, segment_ids, domain_ids, domain_weights, table, attn_weights, out_weights, ffn_weights, down_weights, gains, table_moment, attn_moment, out_moment, ffn_moment, down_moment, gain_moment, table_average, attn_average, out_average, ffn_average, down_average, gain_average):
    masters = (table, attn_weights, out_weights, ffn_weights, down_weights, gains)
    moments = (table_moment, attn_moment, out_moment, ffn_moment, down_moment, gain_moment)
    averages = (table_average, attn_average, out_average, ffn_average, down_average, gain_average)
    matches = (domain_ids.reshape(-1)[:, None] == jnp.arange(DOMAINS)[None, :]).astype(jnp.float32)
    counts = jnp.maximum(lax.optimization_barrier(jnp.sum(matches, axis=0)), 1.0)
    weight_values = domain_weights.astype(jnp.float32)
    total_weight = jnp.sum(weight_values)

    def objective(params):
        lowered = tuple((low(member) for member in params))

        def one_row(carry, row_inputs):
            return (carry + jax.checkpoint(sequence_terms)(lowered, *row_inputs), None)
        sums, _ = lax.scan(one_row, jnp.zeros((DOMAINS,), jnp.float32), (token_ids, target_ids, segment_ids, domain_ids))
        domain_loss = sums / counts
        return (jnp.sum(weight_values * domain_loss) / total_weight, domain_loss)
    total_loss, pullback, domain_loss = jax.vjp(objective, masters, has_aux=True)
    gradients = pullback(jnp.ones_like(total_loss))[0]
    squares = sum((jnp.sum(member * member) for member in gradients))
    grad_norm = jnp.sqrt(squares)
    clip_factor = jnp.minimum(1.0, CLIP_NORM / grad_norm)
    results = [total_loss, domain_loss, grad_norm]
    for master, moment, average, gradient in zip(masters, moments, averages, gradients):
        clipped = gradient * clip_factor
        new_moment = MOMENTUM * moment + clipped
        new_weight = master - LEARN_RATE * (clipped + MOMENTUM * new_moment)
        results.extend([new_moment, new_weight, AVERAGE_KEEP * average + (1.0 - AVERAGE_KEEP) * new_weight])
    return (results[0], results[1], results[2], results[3], results[4], results[5], results[6], results[7], results[8], results[9], results[10], results[11], results[12], results[13], results[14], results[15], results[16], results[17], results[18], results[19], results[20])
```

```python
import functools

import jax
import jax.numpy as jnp
from jax import lax
from jax.experimental import pallas as pl
from jax.experimental.pallas import tpu as pltpu
from jax.sharding import PartitionSpec as P

HD = 64
DOMAINS = 8
SLOTS = 64

EPSILON = 1e-06
CLIP_NORM = 0.01
LEARN_RATE = 1000.0
MOMENTUM = 0.9
AVERAGE_KEEP = 0.75
MASKED = -1e30
MESH = pl.DeviceIdType.MESH
F32 = jnp.float32
BF16 = jnp.bfloat16
VMEM_SPEC = pl.BlockSpec(memory_space=pltpu.VMEM)
ANY_SPEC = pl.BlockSpec(memory_space=pl.ANY)


def rotary_tables(length, half):
    places = jnp.arange(length, dtype=F32)[:, None]
    speeds = 10000.0 ** (-jnp.arange(half, dtype=F32) / half)
    angles = places * speeds
    return (jnp.cos(angles)[:, None, :], jnp.sin(angles)[:, None, :])


def rotate(values, cosine, sine, direction):
    half = values.shape[-1] // 2
    first = values[..., :half]
    second = values[..., half:]
    return jnp.concatenate(
        [first * cosine - direction * second * sine, second * cosine + direction * first * sine],
        axis=-1,
    )


def block_scores(queries, keys, segments, offset, block_rows):
    query_block = lax.dynamic_slice_in_dim(queries, offset, block_rows, 0)
    query_segments = lax.dynamic_slice_in_dim(segments, offset, block_rows, 0)
    places = jnp.arange(segments.shape[0], dtype=jnp.int32)
    query_places = offset + jnp.arange(block_rows, dtype=jnp.int32)
    allowed = (query_places[:, None] >= places[None, :]) & (
        query_segments[:, None] == segments[None, :]
    )
    raw_scores = jnp.einsum(
        "qhd,khd->hqk", query_block, keys, preferred_element_type=F32
    ) * HD ** (-0.5)
    return (jnp.where(allowed[None], raw_scores, MASKED), query_block)


def attend_forward(queries, keys, values, segments, block_rows):
    length = queries.shape[0]

    def one_block(offset):
        scores, query_block = block_scores(queries, keys, segments, offset, block_rows)
        highest = jnp.max(scores, axis=-1, keepdims=True)
        raised = jnp.exp(scores - highest)
        totals = jnp.sum(raised, axis=-1, keepdims=True)
        mixed = jnp.einsum(
            "hqk,khd->qhd", (raised / totals).astype(BF16), values, preferred_element_type=F32
        )
        return (mixed, (highest + jnp.log(totals))[..., 0])

    offsets = jnp.arange(length // block_rows, dtype=jnp.int32) * block_rows
    mixed, log_totals = lax.map(one_block, offsets)
    return (mixed.reshape(length, queries.shape[1], queries.shape[2]), log_totals)


def attend_backward(queries, keys, values, segments, log_totals, out_grad, block_rows):
    length = queries.shape[0]

    def one_block(carry, inputs):
        offset, block_totals = inputs
        key_grad, value_grad = carry
        scores, query_block = block_scores(queries, keys, segments, offset, block_rows)
        grad_block = lax.dynamic_slice_in_dim(out_grad, offset, block_rows, 0)
        soft_probs = jnp.exp(scores - block_totals[..., None])
        prob_grad = jnp.einsum("qhd,khd->hqk", grad_block, values, preferred_element_type=F32)
        inner = jnp.sum(prob_grad * soft_probs, axis=-1, keepdims=True)
        score_grad = (soft_probs * (prob_grad - inner)).astype(BF16)
        query_grad = jnp.einsum(
            "hqk,khd->qhd", score_grad, keys, preferred_element_type=F32
        ) * HD ** (-0.5)
        key_grad = key_grad + jnp.einsum(
            "hqk,qhd->khd", score_grad, query_block, preferred_element_type=F32
        ) * HD ** (-0.5)
        value_grad = value_grad + jnp.einsum(
            "hqk,qhd->khd", soft_probs.astype(BF16), grad_block, preferred_element_type=F32
        )
        return ((key_grad, value_grad), query_grad)

    empty = jnp.zeros(keys.shape, F32)
    offsets = jnp.arange(length // block_rows, dtype=jnp.int32) * block_rows
    (key_grad, value_grad), query_grad = lax.scan(one_block, (empty, empty), (offsets, log_totals))
    return (query_grad.reshape(queries.shape), key_grad, value_grad)


def contract_rows(left, right):
    return lax.dot_general(left, right, (((0,), (0,)), ((), ())), preferred_element_type=F32)


def contract_last(left, right):
    return lax.dot_general(left, right, (((1,), (1,)), ((), ())), preferred_element_type=F32)


def norm_factor(values):
    return lax.rsqrt(jnp.mean(values * values, axis=-1, keepdims=True) + EPSILON)


def norm_back(values, factor, gain, upward):
    gained = gain * upward
    inward = factor * gained - values * (factor * factor * factor) * jnp.mean(
        gained * values, axis=-1, keepdims=True
    )
    return (inward, jnp.sum(upward * values * factor, axis=0, keepdims=True))


def ring_place(member, count):
    odd = lax.rem(member, 2)
    return (1 - odd) * lax.div(member, 2) + odd * (count - 1 - lax.div(member, 2))


def ring_member(place, count):
    back = lax.div(place, count // 2)
    return (1 - back) * (2 * place) + back * (2 * (count - 1 - place) + 1)


def place_block(member, planes):
    return (member % 2) * planes + member // 2


def greet(peers):
    barrier = pltpu.get_barrier_semaphore()
    for peer in peers:
        pl.semaphore_signal(barrier, inc=1, device_id=peer, device_id_type=MESH)
    pl.semaphore_wait(barrier, len(peers))


def send(source, target, send_sem, recv_sem, peer):
    return pltpu.make_async_remote_copy(
        src_ref=source,
        dst_ref=target,
        send_sem=send_sem,
        recv_sem=recv_sem,
        device_id=peer,
        device_id_type=MESH,
    )


def rows_over_mp(name, ident, groups, partials, blocks, vectors, row_fn, outs, sums, gather, tile):
    planes = groups // 2
    count = len(partials)
    if partials:
        rows, width = partials[0].shape[0] // groups, partials[0].shape[1]
    else:
        rows, width = blocks[0].shape
    shaped = [p.reshape(2, planes, rows, width) for p in partials]
    tile = min(tile, rows)

    def body(*refs):
        refs = list(refs)
        take = lambda n: [refs.pop(0) for _ in range(n)]
        part_refs, block_refs, vector_refs = take(count), take(len(blocks)), take(len(vectors))
        out_refs, sum_refs = take(len(outs)), take(sums)
        whole_ref = take(1)[0] if gather else None
        recv_core, recv_plane, send_plane = take(count), take(count), take(count)
        core_sems, plane_sems, near_sems, far_sems = take(4)
        dp = lax.axis_index("dp")
        member = lax.axis_index("mp")
        plane, core = lax.div(member, 2), lax.rem(member, 2)
        partner = (dp, 2 * plane + 1 - core)
        others = [lax.rem(plane + j, planes) for j in range(1, planes)]
        peers = [(dp, 2 * other + core) for other in others]
        greet([partner] + peers)
        copies = []
        for i in range(count):
            copy = send(
                part_refs[i].at[1 - core], recv_core[i], core_sems.at[0, i], core_sems.at[1, i], partner
            )
            copy.start()
            copies.append(copy)
        plane_copies = []
        for i in range(count):
            copies[i].wait_recv()
            for j, other in enumerate(others):

                @pl.loop(0, rows, step=tile)
                def _(r, i=i, j=j, other=other):
                    at = pl.ds(r, tile)
                    send_plane[i][j, at] = (
                        part_refs[i][core, other, at].astype(F32) + recv_core[i][other, at].astype(F32)
                    ).astype(BF16)

                copy = send(
                    send_plane[i].at[j],
                    recv_plane[i].at[j],
                    plane_sems.at[0, i, j],
                    plane_sems.at[1, i, j],
                    peers[j],
                )
                copy.start()
                plane_copies.append(copy)
        for copy in plane_copies:
            copy.wait_recv()
        for ref in sum_refs:
            ref[...] = jnp.zeros_like(ref)

        @pl.loop(0, rows, step=tile)
        def _(r):
            at = pl.ds(r, tile)
            totals = []
            for i in range(count):
                total = part_refs[i][core, plane, at].astype(F32) + recv_core[i][plane, at].astype(F32)
                for j in range(planes - 1):
                    total = total + recv_plane[i][j, at].astype(F32)
                totals.append(total)
            results, sum_parts, gathered = row_fn(
                totals, [ref[at, :] for ref in block_refs], [ref[...] for ref in vector_refs]
            )
            for ref, result in zip(out_refs, results):
                ref[at, :] = result.astype(ref.dtype)
            for ref, part in zip(sum_refs, sum_parts):
                ref[...] += part
            if gather:
                whole_ref[core, plane, at] = gathered.astype(BF16)

        if gather:
            near, far = [], []
            for j in range(planes - 1):
                copy = send(
                    whole_ref.at[core, plane],
                    whole_ref.at[core, plane],
                    far_sems.at[0, j],
                    far_sems.at[1, j],
                    peers[j],
                )
                copy.start()
                far.append(copy)
            for j in range(planes):
                source = lax.rem(plane + planes - j, planes)
                if j:
                    far[j - 1].wait_recv()
                copy = send(
                    whole_ref.at[core, source],
                    whole_ref.at[core, source],
                    near_sems.at[0, j],
                    near_sems.at[1, j],
                    partner,
                )
                copy.start()
                near.append(copy)
            for copy in near:
                copy.wait_recv()
            for copy in near + far:
                copy.wait_send()
        for copy in copies + plane_copies:
            copy.wait_send()

    out_shape = [jax.ShapeDtypeStruct((rows, width), dtype) for dtype in outs]
    out_shape += [jax.ShapeDtypeStruct((1, width), F32)] * sums
    if gather:
        out_shape.append(jax.ShapeDtypeStruct((2, planes, rows, width), BF16))
    far_count = max(planes - 1, 1)
    scratch = [pltpu.VMEM((planes, rows, width), BF16)] * count
    scratch += [pltpu.VMEM((far_count, rows, width), BF16)] * (2 * count)
    scratch += [
        pltpu.SemaphoreType.DMA((2, max(count, 1))),
        pltpu.SemaphoreType.DMA((2, max(count, 1), far_count)),
        pltpu.SemaphoreType.DMA((2, planes)),
        pltpu.SemaphoreType.DMA((2, far_count)),
    ]
    results = pl.pallas_call(
        body,
        name=name,
        out_shape=out_shape,
        in_specs=[VMEM_SPEC] * (count + len(blocks) + len(vectors)),
        out_specs=[VMEM_SPEC] * len(out_shape),
        scratch_shapes=scratch,
        compiler_params=pltpu.CompilerParams(
            collective_id=ident, has_side_effects=True, vmem_limit_bytes=48 * 2**20
        ),
    )(*shaped, *blocks, *vectors)
    results = list(results)
    if gather:
        results[-1] = results[-1].reshape(groups * rows, width)
    return results


def exchange_over_dp(name, ident, values):
    members = values.shape[0]

    def body(in_ref, out_ref, sems):
        dp, mp = lax.axis_index("dp"), lax.axis_index("mp")
        peers = [(lax.rem(dp + k, members), mp) for k in range(1, members)]
        greet(peers)
        copies = []
        for k in range(1, members):
            copy = send(
                in_ref.at[peers[k - 1][0]],
                out_ref.at[dp],
                sems.at[0, k - 1],
                sems.at[1, k - 1],
                peers[k - 1],
            )
            copy.start()
            copies.append(copy)
        out_ref[dp] = in_ref[dp]
        for copy in copies:
            copy.wait_recv()
        for copy in copies:
            copy.wait_send()

    return pl.pallas_call(
        body,
        name=name,
        out_shape=jax.ShapeDtypeStruct(values.shape, values.dtype),
        in_specs=[VMEM_SPEC],
        out_specs=VMEM_SPEC,
        scratch_shapes=[pltpu.SemaphoreType.DMA((2, members - 1))],
        compiler_params=pltpu.CompilerParams(
            collective_id=ident, has_side_effects=True, vmem_limit_bytes=32 * 2**20
        ),
    )(values)


def gather_rows(name, ident, members, groups, block):
    planes = groups // 2
    rows, width = block.shape
    half = planes // 2

    def body(in_ref, out_ref, first_sem, plane_sems, ring_sems, core_sems):
        dp, member = lax.axis_index("dp"), lax.axis_index("mp")
        plane, core = lax.div(member, 2), lax.rem(member, 2)
        place = ring_place(dp, members)
        right = (ring_member(lax.rem(place + 1, members), members), member)
        left = (ring_member(lax.rem(place + members - 1, members), members), member)
        partner = (dp, 2 * plane + 1 - core)
        peers = [(dp, 2 * lax.rem(plane + j, planes) + core) for j in range(1, planes)]
        greet([right, left, partner] + peers)
        own = pltpu.make_async_copy(in_ref, out_ref.at[dp, core, plane], first_sem)
        own.start()
        waits = []
        for j in range(planes - 1):
            copy = send(
                in_ref, out_ref.at[dp, core, plane], plane_sems.at[0, j], plane_sems.at[1, j], peers[j]
            )
            copy.start()
            waits.append(copy)
        own.wait()
        for copy in waits:
            copy.wait_recv()
        ways = ((right, 0, members - 1), (left, 1, 1))

        def piece(source, way):
            return out_ref.at[source, core, pl.ds(way * half, half)]

        def start(k):
            for peer, way, step in ways:
                source = ring_member(lax.rem(place + k * step, members), members)

                @pl.when(k < members - 1)
                def _():
                    send(
                        piece(source, way),
                        piece(source, way),
                        ring_sems.at[0, way, k],
                        ring_sems.at[1, way, k],
                        peer,
                    ).start()

                send(
                    piece(source, way),
                    piece(source, way),
                    core_sems.at[0, way, k],
                    core_sems.at[1, way, k],
                    partner,
                ).start()

        def wait_ring(k):
            for peer, way, step in ways:
                send(
                    piece(dp, way),
                    piece(dp, way),
                    ring_sems.at[0, way, k],
                    ring_sems.at[1, way, k],
                    peer,
                ).wait_recv()

        start(0)

        @pl.loop(1, members)
        def _(k):
            wait_ring(k - 1)
            start(k)

        @pl.loop(0, members)
        def _(k):
            for peer, way, step in ways:
                near = send(
                    piece(dp, way),
                    piece(dp, way),
                    core_sems.at[0, way, k],
                    core_sems.at[1, way, k],
                    partner,
                )
                near.wait_recv()
                near.wait_send()

                @pl.when(k < members - 1)
                def _():
                    send(
                        piece(dp, way),
                        piece(dp, way),
                        ring_sems.at[0, way, k],
                        ring_sems.at[1, way, k],
                        peer,
                    ).wait_send()

        for copy in waits:
            copy.wait_send()

    return pl.pallas_call(
        body,
        name=name,
        out_shape=jax.ShapeDtypeStruct((members, 2, planes, rows, width), block.dtype),
        in_specs=[VMEM_SPEC],
        out_specs=ANY_SPEC,
        scratch_shapes=[
            pltpu.SemaphoreType.DMA,
            pltpu.SemaphoreType.DMA((2, max(planes - 1, 1))),
            pltpu.SemaphoreType.DMA((2, 2, members)),
            pltpu.SemaphoreType.DMA((2, 2, members)),
        ],
        compiler_params=pltpu.CompilerParams(collective_id=ident, has_side_effects=True),
    )(block).reshape(members * groups * rows, width)


def scatter_rows(name, ident, members, groups, values):
    planes = groups // 2
    width = values.shape[1]
    rows = values.shape[0] // (members * groups)
    half = planes // 2
    shaped = values.reshape(members, 2, planes, rows, width)
    tile = min(64, rows)

    def body(
        in_ref,
        out_ref,
        near_ref,
        held,
        going,
        own,
        near,
        last,
        plane_held,
        core_sems,
        ring_sems,
        load_sems,
        plane_sems,
    ):
        dp, member = lax.axis_index("dp"), lax.axis_index("mp")
        plane, core = lax.div(member, 2), lax.rem(member, 2)
        place = ring_place(dp, members)
        right = (ring_member(lax.rem(place + 1, members), members), member)
        left = (ring_member(lax.rem(place + members - 1, members), members), member)
        partner = (dp, 2 * plane + 1 - core)
        others = [lax.rem(plane + j, planes) for j in range(1, planes)]
        peers = [(dp, 2 * other + core) for other in others]
        greet([right, left, partner] + peers)
        ways = ((right, 0, members - 1), (left, 1, 1))

        def target(k, way):
            step = ways[way][2]
            return ring_member(lax.rem(place + (k + 1) * step, members), members)

        def core_copy(k, way):
            block = target(k, way)
            at = pl.ds(way * half, half)
            return send(
                in_ref.at[block, 1 - core, at],
                near_ref.at[block, at],
                core_sems.at[0, way, k],
                core_sems.at[1, way, k],
                partner,
            )

        def loads(k, way):
            block, slot = target(k, way), lax.rem(k, 2)
            at = pl.ds(way * half, half)
            return (
                pltpu.make_async_copy(
                    in_ref.at[block, core, at], own.at[way, slot], load_sems.at[0, way, slot]
                ),
                pltpu.make_async_copy(
                    near_ref.at[block, at], near.at[way, slot], load_sems.at[1, way, slot]
                ),
            )

        def ring_copy(k, way):
            return send(
                going.at[way, lax.rem(k, 2)],
                held.at[way, k],
                ring_sems.at[0, way, k],
                ring_sems.at[1, way, k],
                ways[way][0],
            )

        @pl.loop(0, members)
        def _(k):
            for way in range(2):
                core_copy(k, way).start()

        for way in range(2):
            core_copy(0, way).wait_recv()
            for load in loads(0, way):
                load.start()

        @pl.loop(0, members)
        def _(k):
            slot = lax.rem(k, 2)

            @pl.when(k + 1 < members)
            def _():
                for way in range(2):
                    core_copy(k + 1, way).wait_recv()
                    for load in loads(k + 1, way):
                        load.start()

            for way in range(2):
                for load in loads(k, way):
                    load.wait()

                @pl.when(k >= 2)
                def _():
                    ring_copy(k - 2, way).wait_send()

                @pl.when(k >= 1)
                def _():
                    ring_copy(k - 1, way).wait_recv()

                for b in range(half):

                    @pl.loop(0, rows, step=tile)
                    def _(r):
                        at = pl.ds(r, tile)
                        mine = own[way, slot, b, at].astype(F32) + near[way, slot, b, at].astype(F32)

                        @pl.when(k == 0)
                        def _():
                            going[way, slot, b, at] = mine.astype(BF16)

                        @pl.when(k > 0)
                        def _():
                            came = held[way, jnp.maximum(k - 1, 0), b, at].astype(F32)

                            @pl.when(k < members - 1)
                            def _():
                                going[way, slot, b, at] = (mine + came).astype(BF16)

                            @pl.when(k == members - 1)
                            def _():
                                last[way * half + b, at] = mine + came
                                going[way, slot, b, at] = (mine + came).astype(BF16)

                @pl.when(k < members - 1)
                def _():
                    ring_copy(k, way).start()

        for way in range(2):
            ring_copy(members - 2, way).wait_send()
        final = (members - 1) % 2
        plane_copies = []
        for j, other in enumerate(others):
            copy = send(
                going.at[lax.div(other, half), final, lax.rem(other, half)],
                plane_held.at[j],
                plane_sems.at[0, j],
                plane_sems.at[1, j],
                peers[j],
            )
            copy.start()
            plane_copies.append(copy)

        @pl.loop(0, members)
        def _(k):
            for way in range(2):
                core_copy(k, way).wait_send()

        for copy in plane_copies:
            copy.wait_recv()

        @pl.loop(0, rows, step=tile)
        def _(r):
            at = pl.ds(r, tile)
            total = last[plane, at]
            for j in range(planes - 1):
                total = total + plane_held[j, at].astype(F32)
            out_ref[at, :] = total

        for copy in plane_copies:
            copy.wait_send()

    message = (half, rows, width)
    return pl.pallas_call(
        body,
        name=name,
        out_shape=[
            jax.ShapeDtypeStruct((rows, width), F32),
            jax.ShapeDtypeStruct((members, planes, rows, width), BF16),
        ],
        in_specs=[ANY_SPEC],
        out_specs=[VMEM_SPEC, ANY_SPEC],
        scratch_shapes=[
            pltpu.VMEM((2, members - 1, *message), BF16),
            pltpu.VMEM((2, 2, *message), BF16),
            pltpu.VMEM((2, 2, *message), BF16),
            pltpu.VMEM((2, 2, *message), BF16),
            pltpu.VMEM((planes, rows, width), F32),
            pltpu.VMEM((planes - 1, rows, width), BF16),
            pltpu.SemaphoreType.DMA((2, 2, members)),
            pltpu.SemaphoreType.DMA((2, 2, members - 1)),
            pltpu.SemaphoreType.DMA((2, 2, 2)),
            pltpu.SemaphoreType.DMA((2, planes - 1)),
        ],
        compiler_params=pltpu.CompilerParams(
            collective_id=ident, has_side_effects=True, vmem_limit_bytes=56 * 2**20
        ),
    )(shaped)[0]


def head_forward(hidden, table, places, vocab, tile):
    tokens, width = hidden.shape
    padded = table.shape[0]

    def body(hidden_ref, table_ref, place_ref, raised_ref, high_ref, total_ref, hit_ref):
        logits = contract_last(table_ref[...], hidden_ref[...])
        row = lax.broadcasted_iota(jnp.int32, logits.shape, 0)
        inside = jnp.where(row < vocab, logits, MASKED)
        high = jnp.max(inside, axis=0, keepdims=True)
        raised = jnp.exp(inside - high)
        raised_ref[...] = raised.astype(BF16)
        high_ref[...] = high
        total_ref[...] = jnp.sum(raised, axis=0, keepdims=True)
        hit_ref[...] = jnp.sum(jnp.where(row == place_ref[...], logits, 0.0), axis=0, keepdims=True)

    line = pl.BlockSpec((1, tile), lambda i: (0, i))
    return pl.pallas_call(
        body,
        name="head_forward",
        grid=(tokens // tile,),
        out_shape=[jax.ShapeDtypeStruct((padded, tokens), BF16)]
        + [jax.ShapeDtypeStruct((1, tokens), F32)] * 3,
        in_specs=[
            pl.BlockSpec((tile, width), lambda i: (i, 0)),
            pl.BlockSpec((padded, width), lambda i: (0, 0)),
            line,
        ],
        out_specs=[pl.BlockSpec((padded, tile), lambda i: (0, i)), line, line, line],
        compiler_params=pltpu.CompilerParams(vmem_limit_bytes=58 * 2**20),
    )(hidden, table, places)


def head_backward(raised, scale, coef, places, hidden, table, tile):
    padded, tokens = raised.shape
    width = hidden.shape[1]

    def body(raised_ref, scale_ref, coef_ref, place_ref, hidden_ref, table_ref, back_ref, grad_ref):
        row = lax.broadcasted_iota(jnp.int32, raised_ref.shape, 0)
        hits = jnp.where(row == place_ref[...], coef_ref[...], 0.0)
        slope = (raised_ref[...].astype(F32) * scale_ref[...] - hits).astype(BF16)
        back_ref[...] = contract_rows(slope, table_ref[...]).astype(BF16)
        step = jnp.dot(slope, hidden_ref[...], preferred_element_type=F32)

        @pl.when(pl.program_id(0) == 0)
        def _():
            grad_ref[...] = step

        @pl.when(pl.program_id(0) > 0)
        def _():
            grad_ref[...] += step

    line = pl.BlockSpec((1, tile), lambda i: (0, i))
    return pl.pallas_call(
        body,
        name="head_backward",
        grid=(tokens // tile,),
        out_shape=[
            jax.ShapeDtypeStruct((tokens, width), BF16),
            jax.ShapeDtypeStruct((padded, width), F32),
        ],
        in_specs=[
            pl.BlockSpec((padded, tile), lambda i: (0, i)),
            line,
            line,
            line,
            pl.BlockSpec((tile, width), lambda i: (i, 0)),
            pl.BlockSpec((padded, width), lambda i: (0, 0)),
        ],
        out_specs=[
            pl.BlockSpec((tile, width), lambda i: (i, 0)),
            pl.BlockSpec((padded, width), lambda i: (0, 0)),
        ],
        compiler_params=pltpu.CompilerParams(vmem_limit_bytes=58 * 2**20),
    )(raised, scale, coef, places, hidden, table)


def one_hot(indices, size):
    return (indices[:, None] == jnp.arange(size, dtype=jnp.int32)[None, :]).astype(BF16)


def slots_of(ids, shard):
    length = ids.shape[0]
    owners = ids // shard
    order = jnp.arange(length, dtype=jnp.int32)
    same = ids[:, None] == ids[None, :]
    again = jnp.any(same & (order[None, :] < order[:, None]), axis=1)
    ahead = (owners[:, None] == owners[None, :]) & (ids[None, :] < ids[:, None]) & ~again[None, :]
    return jnp.sum(ahead.astype(jnp.int32), axis=1)


def per_device(
    members,
    groups,
    token_ids,
    target_ids,
    segment_ids,
    domain_ids,
    domain_weights,
    table,
    attn_weights,
    out_weights,
    ffn_weights,
    down_weights,
    gains,
    table_moment,
    attn_moment,
    out_moment,
    ffn_moment,
    down_moment,
    gain_moment,
    table_average,
    attn_average,
    out_average,
    ffn_average,
    down_average,
    gain_average,
):
    masters = (table, attn_weights, out_weights, ffn_weights, down_weights, gains)
    moments = (table_moment, attn_moment, out_moment, ffn_moment, down_moment, gain_moment)
    averages = (table_average, attn_average, out_average, ffn_average, down_average, gain_average)
    planes = groups // 2
    dp, member = lax.axis_index("dp"), lax.axis_index("mp")
    device = dp * groups + member
    block = place_block(member, planes)
    tokens, segments = token_ids[0], segment_ids[0]
    length = tokens.shape[0]
    vocab, width = table.shape
    rows = length // groups
    padded = -(-vocab // 16) * 16

    square = lax.all_gather(
        jnp.concatenate([attn_weights, out_weights.T[None]]).astype(BF16), "dp", axis=1, tiled=True
    )
    long = lax.all_gather(
        jnp.concatenate([ffn_weights, down_weights.T[None]]).astype(BF16), "dp", axis=1, tiled=True
    )
    gain_full = lax.all_gather(gains.astype(BF16), "dp", axis=1, tiled=True).astype(F32)
    gain_rows = [gain_full[i : i + 1] for i in range(4)]
    table_low = jnp.pad(table.astype(BF16), ((0, padded - vocab), (0, 0)))

    slots = slots_of(tokens, vocab)
    known = lax.all_gather(
        jnp.stack([tokens, target_ids[0], domain_ids[0], slots]), "dp", axis=0, tiled=False
    )
    all_ids, all_targets, all_domains, all_slots = (known[:, i] for i in range(4))
    fits = jnp.all(all_slots < SLOTS)
    owners = tokens // vocab
    spots = (
        place_block(owners % groups, planes) * (members * SLOTS) + owners // groups * SLOTS + slots
    )

    def sparse_rows():
        mine = all_ids // vocab == device
        slot = jnp.arange(SLOTS, dtype=jnp.int32)
        wanted = jnp.max(
            jnp.where(
                mine[:, :, None] & (all_slots[:, :, None] == slot), (all_ids % vocab)[:, :, None], -1
            ),
            axis=1,
        ).reshape(-1)
        chosen = jnp.dot(one_hot(wanted, padded), table_low)
        came = exchange_over_dp("embed_dp", 1, chosen.reshape(members, SLOTS, width))
        came = came.reshape(members * SLOTS, width)
        whole = rows_over_mp(
            "embed_mp", 2, groups, [], [came], [], lambda t, b, v: ([], [], b[0]), [], 0, True, 64
        )[0]
        return jnp.dot(one_hot(spots, groups * members * SLOTS), whole)

    def dense_rows():
        flat = all_ids.reshape(-1)
        picked = jnp.take(table_low, flat % vocab, axis=0)
        picked = jnp.where((flat // vocab == device)[:, None], picked, jnp.zeros_like(picked))
        return lax.psum(
            lax.psum_scatter(picked, "dp", scatter_dimension=0, tiled=True), "mp"
        )

    embedded_low = lax.cond(fits, sparse_rows, dense_rows)
    embedded = embedded_low.astype(F32)
    own_rows = lax.dynamic_slice_in_dim(embedded, block * rows, rows, 0)

    cosine, sine = rotary_tables(length, HD // 2)
    factor = norm_factor(embedded)
    first_low = (embedded * factor * gain_rows[0]).astype(BF16)
    attn_low = (embedded * factor * gain_rows[1]).astype(BF16)
    value_first = jnp.dot(first_low, square[3], preferred_element_type=F32).astype(BF16)
    projected = jnp.einsum("td,kdc->ktc", attn_low, square[:3], preferred_element_type=F32)
    columns = square.shape[2]
    heads = columns // HD
    queries = rotate(projected[0].reshape(length, heads, HD), cosine, sine, 1.0).astype(BF16)
    keys = rotate(projected[1].reshape(length, heads, HD), cosine, sine, 1.0).astype(BF16)
    values = (
        (0.5 * projected[2] + 0.5 * value_first.astype(F32)).astype(BF16).reshape(length, heads, HD)
    )
    block_rows = min(512, length)
    mixed, log_totals = attend_forward(queries, keys, values, segments, block_rows)
    mixed_low = mixed.reshape(length, columns).astype(BF16)
    out_part = contract_last(mixed_low, square[4]).astype(BF16)

    def after_attention(totals, blocks, vectors):
        residual = blocks[0] + totals[0]
        return ([residual], [], residual * norm_factor(residual) * vectors[0])

    residual_one, ffn_low = rows_over_mp(
        "after_attention", 3, groups, [out_part], [own_rows], [gain_rows[2]], after_attention,
        [F32], 0, True, 64,
    )

    gate_up = jnp.einsum("td,kdf->ktf", ffn_low, long[:2], preferred_element_type=F32)
    sigmoid_gate = jax.nn.sigmoid(gate_up[0])
    silu_gate = gate_up[0] * sigmoid_gate
    activated = (silu_gate * gate_up[1]).astype(BF16)
    down_part = contract_last(activated, long[2]).astype(BF16)

    def after_ffn(totals, blocks, vectors):
        residual = blocks[0] + totals[0]
        return ([residual, residual * norm_factor(residual) * vectors[0]], [], None)

    residual_two, final_low = rows_over_mp(
        "after_ffn", 4, groups, [down_part], [residual_one], [gain_rows[3]], after_ffn,
        [F32, BF16], 0, False, 64,
    )

    hidden = gather_rows("gather_hidden", 5, members, groups, final_low)
    flat_targets = all_targets.reshape(1, -1)
    places = jnp.where(flat_targets // vocab == device, flat_targets % vocab, -1)
    tile = min(512, length)
    raised, high, total, hit = head_forward(hidden, table_low, places, vocab, tile)
    row_high = lax.pmax(high, ("dp", "mp"))
    row_total, target_total = lax.psum(
        (total * jnp.exp(high - row_high), hit), ("dp", "mp")
    )
    row_lse = row_high + jnp.log(row_total)
    token_loss = (row_lse - target_total)[0]
    matches = (
        all_domains.reshape(-1)[:, None] == jnp.arange(DOMAINS, dtype=jnp.int32)[None, :]
    ).astype(F32)
    counts = jnp.maximum(jnp.sum(matches, axis=0), 1.0)
    domain_loss = jnp.sum(matches * token_loss[:, None], axis=0) / counts
    weight_values = domain_weights.astype(F32)
    total_weight = jnp.sum(weight_values)
    total_loss = jnp.sum(weight_values * domain_loss) / total_weight
    coef = jnp.sum(matches * (weight_values / total_weight / counts)[None, :], axis=1)[None, :]
    scale = coef * jnp.exp(high - row_lse)
    hidden_back, table_head = head_backward(raised, scale, coef, places, hidden, table_low, tile)
    final_grad = scatter_rows("scatter_hidden", 6, members, groups, hidden_back)

    def before_head(totals, blocks, vectors):
        grad, final_gain = norm_back(blocks[1], norm_factor(blocks[1]), vectors[0], blocks[0])
        return ([grad], [final_gain], grad)

    two_grad, final_gain, down_in = rows_over_mp(
        "before_head", 7, groups, [], [final_grad, residual_two], [gain_rows[3]], before_head,
        [F32], 1, True, 64,
    )

    down_grad = contract_rows(down_in, activated)
    act_grad = jnp.dot(down_in, long[2], preferred_element_type=F32)
    gate_grad = act_grad * gate_up[1] * sigmoid_gate * (1.0 + gate_up[0] * (1.0 - sigmoid_gate))
    pair_grad = jnp.stack([gate_grad, act_grad * silu_gate]).astype(BF16)
    ffn_part = jnp.einsum(
        "ktf,kdf->td", pair_grad, long[:2], preferred_element_type=F32
    ).astype(BF16)

    def before_ffn(totals, blocks, vectors):
        inward, ffn_gain = norm_back(blocks[0], norm_factor(blocks[0]), vectors[0], totals[0])
        grad = blocks[1] + inward
        return ([grad], [ffn_gain], grad)

    one_grad, ffn_gain, attn_out = rows_over_mp(
        "before_ffn", 8, groups, [ffn_part], [residual_one, two_grad], [gain_rows[2]], before_ffn,
        [F32], 1, True, 64,
    )
    ffn_grad = jnp.einsum("td,ktf->kdf", ffn_low, pair_grad, preferred_element_type=F32)
    long_sum = lax.psum_scatter(
        jnp.concatenate([ffn_grad, down_grad[None]]).astype(BF16), "dp", scatter_dimension=1, tiled=True
    ).astype(F32)

    out_grad = contract_rows(attn_out, mixed_low)
    mixed_grad = (
        jnp.dot(attn_out, square[4], preferred_element_type=F32).astype(BF16).reshape(length, heads, HD)
    )
    query_grad, key_grad, value_grad = attend_backward(
        queries, keys, values, segments, log_totals, mixed_grad, block_rows
    )
    half_value = (value_grad * 0.5).astype(BF16).reshape(length, columns)
    query_raw = rotate(query_grad, cosine, sine, -1.0).reshape(length, columns).astype(BF16)
    key_raw = rotate(key_grad, cosine, sine, -1.0).reshape(length, columns).astype(BF16)
    triple_grad = jnp.stack([query_raw, key_raw, half_value])
    attn_part = jnp.einsum(
        "ktc,kdc->td", triple_grad, square[:3], preferred_element_type=F32
    ).astype(BF16)
    first_part = contract_last(half_value, square[3]).astype(BF16)

    def before_attention(totals, blocks, vectors):
        factor = norm_factor(blocks[0])
        attn_inward, attn_gain = norm_back(blocks[0], factor, vectors[1], totals[0])
        first_inward, first_gain = norm_back(blocks[0], factor, vectors[0], totals[1])
        return ([], [first_gain, attn_gain], blocks[1] + attn_inward + first_inward)

    first_gain, attn_gain, embed_grad = rows_over_mp(
        "before_attention", 9, groups, [attn_part, first_part], [own_rows, one_grad],
        [gain_rows[0], gain_rows[1]], before_attention, [], 2, True, 64,
    )
    attn_grad = jnp.concatenate(
        [
            jnp.einsum("td,ktc->kdc", attn_low, triple_grad, preferred_element_type=F32),
            contract_rows(first_low, half_value)[None],
            out_grad[None],
        ]
    )
    square_sum = lax.psum_scatter(
        attn_grad.astype(BF16), "dp", scatter_dimension=1, tiled=True
    ).astype(F32)

    def sparse_table():
        first_spot = block * (members * SLOTS)
        places = first_spot + jnp.arange(members * SLOTS, dtype=jnp.int32)
        leaving = jnp.dot(
            (places[:, None] == spots[None, :]).astype(BF16), embed_grad, preferred_element_type=F32
        ).astype(BF16)
        came = exchange_over_dp("table_dp", 10, leaving.reshape(members, SLOTS, width))
        mine = all_ids // vocab == device
        slot = jnp.arange(SLOTS, dtype=jnp.int32)
        wanted = jnp.max(
            jnp.where(
                mine[:, :, None] & (all_slots[:, :, None] == slot), (all_ids % vocab)[:, :, None], -1
            ),
            axis=1,
        ).reshape(-1)
        place = jnp.arange(vocab, dtype=jnp.int32)
        return jnp.dot(
            (place[:, None] == wanted[None, :]).astype(BF16),
            came.reshape(members * SLOTS, width),
            preferred_element_type=F32,
        )

    def dense_table():
        everything = lax.all_gather(embed_grad, "dp", axis=0, tiled=True).astype(F32)
        flat = all_ids.reshape(-1)
        spot = jnp.where(flat // vocab == device, flat % vocab, vocab)
        return jax.ops.segment_sum(everything, spot, num_segments=vocab)

    table_sum = table_head[:vocab] + lax.cond(fits, sparse_table, dense_table)
    gain_grad = lax.psum(
        jnp.concatenate([first_gain, attn_gain, ffn_gain, final_gain]), ("dp", "mp")
    )
    gain_width = gains.shape[1]
    gain_sum = lax.dynamic_slice_in_dim(gain_grad, dp * gain_width, gain_width, 1)
    summed = (table_sum, square_sum[:4], square_sum[4].T, long_sum[:2], long_sum[2].T, gain_sum)
    gain_share = jnp.where(member == 0, 1.0, 0.0)
    squares = sum((jnp.sum(part * part) for part in summed[:5])) + gain_share * jnp.sum(
        summed[5] * summed[5]
    )
    grad_norm = jnp.sqrt(lax.psum(squares, ("dp", "mp")))
    clip_factor = jnp.minimum(1.0, CLIP_NORM / grad_norm)
    results = [total_loss, domain_loss, grad_norm]
    for master, moment, average, gradient in zip(masters, moments, averages, summed):
        clipped = gradient * clip_factor
        new_moment = MOMENTUM * moment + clipped
        new_weight = master - LEARN_RATE * (clipped + MOMENTUM * new_moment)
        results.extend(
            [new_moment, new_weight, AVERAGE_KEEP * average + (1.0 - AVERAGE_KEEP) * new_weight]
        )
    return tuple(results)


def solution(mesh):
    rows = P(("dp", "mp"), None)
    cube = P(None, "dp", "mp")
    down = P("mp", "dp")
    gain = P(None, "dp")
    ids = P("dp", None)
    state = (rows, cube, down, cube, down, gain)
    return jax.shard_map(
        functools.partial(per_device, mesh.shape["dp"], mesh.shape["mp"]),
        mesh=mesh,
        in_specs=(ids, ids, ids, ids, P(), *state, *state, *state),
        out_specs=(P(), P(), P(), *(spec for spec in state for _ in range(3))),
        check_vma=False,
    )
```
